64 devices in a mesh: rep: 4 (over x, y), dp: 16 (over z, core).
Axes of the slice: x: 2, y: 2, z: 8, core: 2. Of those that a mesh axis runs over, the one named last changes fastest.
The devices are a block of a 4x4x8 slice.
Arguments:
- x: bfloat16 [64, 2048, 640], P(('rep', 'dp')), parts along dimension 0
- dy: bfloat16 [64, 2048, 640], P(('rep', 'dp')), parts along dimension 0
- w_gate: bfloat16 [2, 640, 2048], P(None, 'dp')
- w_up: bfloat16 [2, 640, 2048], P(None, 'dp')
- w_down: bfloat16 [2, 2048, 640], P(None, 'dp')
- m_w_gate: float32 [2, 640, 2048], P(None, 'dp')
- m_w_up: float32 [2, 640, 2048], P(None, 'dp')
- m_w_down: float32 [2, 2048, 640], P(None, 'dp')
- v_w_gate: float32 [2, 640, 2048], P(None, 'dp')
- v_w_up: float32 [2, 640, 2048], P(None, 'dp')
- v_w_down: float32 [2, 2048, 640], P(None, 'dp')
Outputs:
- output 1: bfloat16 [8, 640, 2048], P('rep', 'dp'), parts along dimension 0
- output 2: bfloat16 [8, 640, 2048], P('rep', 'dp'), parts along dimension 0
- output 3: bfloat16 [8, 2048, 640], P('rep', 'dp'), parts along dimension 0
- output 4: float32 [8, 640, 2048], P('rep', 'dp'), parts along dimension 0
- output 5: float32 [8, 640, 2048], P('rep', 'dp'), parts along dimension 0
- output 6: float32 [8, 2048, 640], P('rep', 'dp'), parts along dimension 0
- output 7: float32 [8, 640, 2048], P('rep', 'dp'), parts along dimension 0
- output 8: float32 [8, 640, 2048], P('rep', 'dp'), parts along dimension 0
- output 9: float32 [8, 2048, 640], P('rep', 'dp'), parts along dimension 0
There are 4 independent parts. The reference program is written for one: setup_inputs(seed, part) draws one part's arguments, and reference() takes and returns one part's arrays. A program takes and returns all parts, laid end to end along the dimension named above; an argument that names none is the same for every part.
All inputs are finite; a program needn't handle non-finite values.
Results may differ from the reference program's by a relative error of at most 0.0228.
Values are sent between devices in bfloat16 or wider.
A program may use at most 768 MiB of HBM per device.

```python
import jax
import jax.numpy as jnp
from jax import lax

SEQUENCES = 16
TOKENS = 2048
D = 640
FF = 2048
LAYERS = 2
NAMES = ("w_gate", "w_up", "w_down")
SHAPES = {"w_gate": (LAYERS, D, FF), "w_up": (LAYERS, D, FF), "w_down": (LAYERS, FF, D)}


def bump(key, n, height):
    away = (jnp.arange(n, dtype=jnp.int32) - jax.random.randint(key, (), 0, n, jnp.int32)) % n
    return jnp.where(away < n // 8, height, 1.0)


def together(key, own, strength):
    shared = jax.random.normal(key, own.shape[1:], jnp.float32)
    return (own + strength * shared) * lax.rsqrt(1 + strength * strength)


def setup_inputs(seed: int = 0, part: int = 0) -> dict:
    kx, kdy, ka, kb, kz, kf, kh, kl, *keys = jax.random.split(jax.random.key(seed), 8 + 3 * len(NAMES))
    kx, kdy, ka, kb = (jax.random.fold_in(k, part) for k in (kx, kdy, ka, kb))
    kw, km, kv = (keys[i::3] for i in range(3))
    shape = (SEQUENCES, TOKENS, D)
    much_x, much_dy = jax.random.uniform(kz, (2,), jnp.float32, 0.0, 1.0)
    loud = 2.0 ** jax.random.uniform(jax.random.fold_in(kz, 1), (), jnp.float32, -1.0, 2.0)
    layers = 2.0 ** jax.random.uniform(kl, (LAYERS, 1, 1), jnp.float32, -1.0, 1.0)
    x = together(ka, jax.random.normal(kx, shape, jnp.float32), much_x) * bump(kf, D, 4.0)
    dy = together(kb, jax.random.normal(kdy, shape, jnp.float32), much_dy)
    drawn = {"x": x.astype(jnp.bfloat16), "dy": (loud * dy * (SEQUENCES * TOKENS) ** -0.5).astype(jnp.bfloat16)}
    for key, name in zip(kw, NAMES, strict=True):
        w = jax.random.normal(key, SHAPES[name], jnp.float32) * SHAPES[name][1] ** -0.5
        drawn[name] = (w * {"w_gate": 1.0, "w_up": bump(kh, FF, 4.0), "w_down": layers}[name]).astype(jnp.bfloat16)
    for key, name in zip(km, NAMES, strict=True):
        drawn[f"m_{name}"] = 0.1 * jax.random.normal(key, SHAPES[name], jnp.float32)
    for key, name in zip(kv, NAMES, strict=True):
        drawn[f"v_{name}"] = jax.random.uniform(key, SHAPES[name], jnp.float32, 0.005, 0.015)
    return drawn


def matmul(a, w):
    return jnp.dot(a, w, preferred_element_type=jnp.float32).astype(jnp.bfloat16)


def normed(h):
    wide = h.astype(jnp.float32)
    scale = lax.rsqrt(jnp.mean(wide**2, -1, keepdims=True) + 1e-6)
    return (wide * scale).astype(jnp.bfloat16)


def layer(h, w):
    a = normed(h)
    gate = jnp.dot(a, w["w_gate"], preferred_element_type=jnp.float32)
    up = jnp.dot(a, w["w_up"], preferred_element_type=jnp.float32)
    return h + matmul((jax.nn.silu(gate) * up).astype(jnp.bfloat16), w["w_down"])


def adamw(w, m, v, g):
    m = 0.9 * m + 0.1 * g
    v = 0.95 * v + 0.05 * g * g
    step = m * lax.rsqrt(v + 1e-8) + 0.1 * w
    return (w - 0.02 * step).astype(jnp.bfloat16), m, v


def clipped(gradients, sum_of_squares, count):
    factor = jnp.minimum(1.0, 0.5 * lax.rsqrt(sum_of_squares / count + 1e-30))
    return [g * factor for g in gradients]


def stack(weights, h):
    return lax.scan(lambda h, w: (layer(h, w), None), h, weights)[0]


def reference(x, dy, w_gate, w_up, w_down, m_w_gate, m_w_up, m_w_down, v_w_gate, v_w_up, v_w_down):
    weights = dict(zip(NAMES, (w_gate, w_up, w_down), strict=True))

    def take(so_far, sequence):
        h, by_y = sequence
        _, back = jax.vjp(lambda w: stack(w, h), weights)
        return jax.tree.map(lambda total, term: total + term.astype(jnp.float32), so_far, back(by_y)[0]), None

    none_yet = {name: jnp.zeros(w.shape, jnp.float32) for name, w in weights.items()}
    by_weights, _ = lax.scan(take, none_yet, (x, dy))
    gradients = [by_weights[name].astype(jnp.bfloat16).astype(jnp.float32) for name in NAMES]
    gradients = clipped(gradients, sum(jnp.sum(g * g) for g in gradients), sum(g.size for g in gradients))
    new = [
        adamw(w.astype(jnp.float32), m, v, g)
        for w, m, v, g in zip((w_gate, w_up, w_down), (m_w_gate, m_w_up, m_w_down), (v_w_gate, v_w_up, v_w_down), gradients, strict=True)
    ]
    return tuple(one[which] for which in range(3) for one in new)
```

```python
import functools

import jax
import jax.numpy as jnp
from jax import lax
from jax.experimental import pallas as pl
from jax.experimental.pallas import tpu as pltpu
from jax.sharding import PartitionSpec as P

BF, F32 = jnp.bfloat16, jnp.float32
MESH = pl.DeviceIdType.MESH
VMEM_LIMIT = 67_000_000
NT = (((1,), (1,)), ((), ()))


def normed(wide):
    scale = lax.rsqrt(jnp.mean(wide * wide, -1, keepdims=True) + 1e-6)
    return (wide * scale).astype(BF)


def dot(a, b):
    return jnp.dot(a, b, preferred_element_type=F32)


def dot_nt(a, b):
    return lax.dot_general(a, b, NT, preferred_element_type=F32)


class Place:
    def __init__(self, n):
        self.n, self.chips = n, n // 2
        self.me = lax.axis_index("dp")
        self.core = lax.rem(self.me, 2)
        self.chip = lax.div(self.me, 2)
        self.partner = self.chip * 2 + (1 - self.core)

    def at(self, offset):
        return lax.rem(self.chip + offset + self.chips, self.chips)

    def device(self, offset):
        return self.at(offset) * 2 + self.core


def greet(devices):
    barrier = pltpu.get_barrier_semaphore()
    for device in devices:
        pl.semaphore_signal(barrier, inc=1, device_id={"dp": device}, device_id_type=MESH)
    pl.semaphore_wait(barrier, len(devices))


def remote(src, dst, send, recv, device):
    return pltpu.make_async_remote_copy(
        src_ref=src, dst_ref=dst, send_sem=send, recv_sem=recv, device_id={"dp": device}, device_id_type=MESH
    )


class Gather:
    def __init__(self, place, shards, fulls, sems):
        self.p, self.shards, self.fulls = place, shards, fulls
        self.local, self.rs, self.rr, self.ps, self.pr = sems
        self.half_hops = place.chips // 2

    @staticmethod
    def sems(n, pieces):
        return [
            pltpu.SemaphoreType.DMA((pieces,)),
            pltpu.SemaphoreType.DMA((pieces, 2, n // 4)),
            pltpu.SemaphoreType.DMA((pieces, 2, n // 4)),
            pltpu.SemaphoreType.DMA((pieces, n // 2)),
            pltpu.SemaphoreType.DMA((pieces, n // 2)),
        ]

    def half(self, ref, h):
        rows, cols = ref.shape
        if cols > rows * 8:
            return ref.at[:, h * (cols // 2) : (h + 1) * (cols // 2)]
        return ref.at[h * (rows // 2) : (h + 1) * (rows // 2), :]

    def hop(self, i, way, t):
        p, full = self.p, self.fulls[i]
        behind = (1 - t) if way == 0 else (t - 1)
        ref = full.at[p.device(behind)]
        if t == self.half_hops:
            ref = self.half(ref, way)
        return remote(ref, ref, self.rs.at[i, way, t - 1], self.rr.at[i, way, t - 1], p.device(1 if way == 0 else -1))

    def landed(self, i, way, t):
        p, full = self.p, self.fulls[i]
        ref = full.at[p.device(-t if way == 0 else t)]
        if t == self.half_hops:
            ref = self.half(ref, way)
        return remote(ref, ref, self.rs.at[i, way, t - 1], self.rr.at[i, way, t - 1], p.device(1))

    def hand(self, i, k):
        p, full = self.p, self.fulls[i]
        offset = 0 if k == 0 else (-(k + 1) // 2 if k % 2 else k // 2)
        ref = full.at[p.device(offset)]
        return remote(ref, ref, self.ps.at[i, k], self.pr.at[i, k], p.partner)

    def handed(self, i, k):
        p, full = self.p, self.fulls[i]
        offset = 0 if k == 0 else (-(k + 1) // 2 if k % 2 else k // 2)
        ref = full.at[p.at(offset) * 2 + (1 - p.core)]
        return remote(ref, ref, self.ps.at[i, k], self.pr.at[i, k], p.partner)

    def begin(self):
        own = [pltpu.make_async_copy(s, f.at[self.p.me], self.local.at[i]) for i, (s, f) in enumerate(zip(self.shards, self.fulls))]
        for c in own:
            c.start()
        for i, c in enumerate(own):
            c.wait()
            self.hop(i, 0, 1).start()
            self.hop(i, 1, 1).start()
            self.hand(i, 0).start()

    def events(self):
        return [(t, i) for t in range(1, self.half_hops + 1) for i in range(len(self.fulls))]

    def forward(self, t, i):
        last = self.half_hops
        for way in range(2):
            self.landed(i, way, t).wait_recv()
            if t < last:
                self.hop(i, way, t + 1).start()
                self.hand(i, 2 * t - 1 + way).start()
        if t == last:
            self.hand(i, 2 * last - 1).start()

    def finish(self):
        for i in range(len(self.fulls)):
            for k in range(self.p.chips):
                self.handed(i, k).wait_recv()
        for i in range(len(self.fulls)):
            for k in range(self.p.chips):
                self.hand(i, k).wait_send()
            for way in range(2):
                for t in range(1, self.half_hops + 1):
                    self.hop(i, way, t).wait_send()


def gather_kernel(n, layer, wg, wu, wd, fg, fu, fd, *sems):
    p = Place(n)
    greet([p.device(1), p.device(-1), p.partner])
    g = Gather(p, [w.at[layer] for w in (wg, wu, wd)], [fg, fu, fd], sems)
    g.begin()
    for t, i in g.events():
        g.forward(t, i)
    g.finish()


def forward_kernel(n, layer, tile, x, wg, wu, wd, sg, su, sd, y, fg, fu, fd, *sems):
    p = Place(n)
    greet([p.device(1), p.device(-1), p.partner])
    g = Gather(p, [w.at[layer] for w in (sg, su, sd)], [fg, fu, fd], sems)
    g.begin()
    events = g.events()
    tiles = x.shape[0] // tile
    ff = wg.shape[1]
    width = 512

    def body(i, _):
        rows = pl.ds(pl.multiple_of(i * tile, tile), tile)
        h = x[rows, :]
        a = normed(h.astype(F32))
        out = None
        for c in range(0, ff, width):
            gate = dot(a, wg[:, c : c + width])
            up = dot(a, wu[:, c : c + width])
            hid = (gate * jax.nn.sigmoid(gate) * up).astype(BF)
            term = dot(hid, wd[c : c + width, :])
            out = term if out is None else out + term
        y[rows, :] = h + out.astype(BF)
        for k, (t, j) in enumerate(events):
            @pl.when(i == k)
            def _(t=t, j=j):
                g.forward(t, j)
        return 0

    lax.fori_loop(0, tiles, body, 0)
    for t, j in events[tiles:]:
        g.forward(t, j)
    g.finish()


class Scatter:
    def __init__(self, place, refs, sems):
        self.p = place
        self.g_gu, self.q_gu, self.s_gu, self.r_gu, self.g_wd, self.q_wd, self.s_wd, self.r_wd = refs
        self.ss_gu, self.sr_gu, self.ss_wd, self.sr_wd, self.ps, self.pr = sems

    @staticmethod
    def scratch(n, gu, wd):
        chips = n // 2
        return [
            pltpu.VMEM((chips, chips, 2) + gu, BF),
            pltpu.VMEM((chips, chips) + gu, BF),
            pltpu.VMEM((chips, 2, 4) + gu, BF),
            pltpu.VMEM((chips, 2, 4) + gu, BF),
            pltpu.VMEM((chips, 2) + wd, BF),
            pltpu.VMEM((chips,) + wd, BF),
            pltpu.VMEM((chips, 2) + wd, BF),
            pltpu.VMEM((chips, 2) + wd, BF),
            pltpu.SemaphoreType.DMA((chips, 2, 4)),
            pltpu.SemaphoreType.DMA((chips, 2, 4)),
            pltpu.SemaphoreType.DMA((chips, 2)),
            pltpu.SemaphoreType.DMA((chips, 2)),
            pltpu.SemaphoreType.DMA((chips, 2)),
            pltpu.SemaphoreType.DMA((chips, 2)),
        ]

    def owner(self, b):
        half = self.p.chips // 2
        return lax.div(b, 2) + half * lax.rem(b, 2)

    def pair(self, b):
        p = self.p
        return [
            remote(self.g_gu.at[b, :, 1 - p.core], self.q_gu.at[b], self.ps.at[b, 0], self.pr.at[b, 0], p.partner),
            remote(self.g_wd.at[b, 1 - p.core], self.q_wd.at[b], self.ps.at[b, 1], self.pr.at[b, 1], p.partner),
        ]

    def own_gu(self, b, chip, cols):
        return self.g_gu[b, chip, self.p.core, :, cols].astype(F32) + self.q_gu[b, chip, :, cols].astype(F32)

    def own_wd(self, b, rows):
        return self.g_wd[b, self.p.core, rows, :].astype(F32) + self.q_wd[b, rows, :].astype(F32)

    def gu_copy(self, b, way, s):
        src, dst = self.s_gu.at[b, way, s], self.r_gu.at[b, way, s]
        if s == 0:
            w = src.shape[1] // 2
            src, dst = (r.at[:, way * w : (way + 1) * w] for r in (src, dst))
        return remote(src, dst, self.ss_gu.at[b, way, s], self.sr_gu.at[b, way, s], self.p.device(1 if way == 0 else -1))

    def wd_copy(self, b, way, first):
        src, dst = self.s_wd.at[b, way], self.r_wd.at[b, way]
        if first:
            h = src.shape[0] // 2
            src, dst = (r.at[way * h : (way + 1) * h, :] for r in (src, dst))
        return remote(src, dst, self.ss_wd.at[b, way], self.sr_wd.at[b, way], self.p.device(1 if way == 0 else -1))

    def stage(self, b, s):
        p = self.p
        if s == 0:
            for c in self.pair(b):
                c.wait_recv()
        width, height = self.g_gu.shape[-1] // 2, self.g_wd.shape[-2] // 2
        for way in range(2):
            far = 4 - s
            chip = p.at(far if way == 0 else -far)
            if s > 0:
                self.gu_copy(b, way, s - 1).wait_recv()
            for h in range(2):
                cols = slice(h * width, (h + 1) * width)
                if s == 0 and h != way:
                    continue
                term = self.own_gu(b, chip, cols)
                if s > 1 or (s == 1 and h == way):
                    term = term + self.r_gu[b, way, s - 1, :, cols].astype(F32)
                self.s_gu[b, way, s, :, cols] = term.astype(BF)
            self.gu_copy(b, way, s).start()

        owner = self.owner(b)
        for way in range(2):
            far = 4 - s

            @pl.when(owner == p.at(far if way == 0 else -far))
            def _(way=way):
                if s > 0:
                    self.wd_copy(b, way, s == 1).wait_recv()
                for h in range(2):
                    rows = slice(h * height, (h + 1) * height)
                    if s == 0 and h != way:
                        continue
                    term = self.own_wd(b, rows)
                    if s > 1 or (s == 1 and h == way):
                        term = term + self.r_wd[b, way, rows, :].astype(F32)
                    self.s_wd[b, way, rows, :] = term.astype(BF)
                self.wd_copy(b, way, s == 0).start()

    def last(self, b, out_gu, out_wd):
        p = self.p
        owner = self.owner(b)
        full = slice(None)
        width = self.g_gu.shape[-1]
        for way in range(2):
            self.gu_copy(b, way, 3).wait_recv()
        total = self.own_gu(b, p.chip, full) + self.r_gu[b, 0, 3].astype(F32) + self.r_gu[b, 1, 3].astype(F32)
        out_gu[:, pl.ds(pl.multiple_of(owner * width, width), width)] = total.astype(BF)

        @pl.when(owner == p.chip)
        def _():
            for way in range(2):
                self.wd_copy(b, way, False).wait_recv()
            out_wd[...] = (self.own_wd(b, full) + self.r_wd[b, 0].astype(F32) + self.r_wd[b, 1].astype(F32)).astype(BF)

    def drain(self):
        p = self.p

        def body(b, _):
            for c in self.pair(b):
                c.wait_send()
            owner = self.owner(b)
            for way in range(2):
                for s in range(4):
                    self.gu_copy(b, way, s).wait_send()
                    far = 4 - s

                    @pl.when(owner == p.at(far if way == 0 else -far))
                    def _(way=way, s=s):
                        self.wd_copy(b, way, s == 0).wait_send()
            return 0

        lax.fori_loop(0, p.chips, body, 0)


def backward_kernel(n, tile, final, *refs):
    refs = list(refs)
    take = lambda k: [refs.pop(0) for _ in range(k)]
    h, dy, wg, wu, wd = take(5)
    before = take(2) if final else []
    out_gu, out_wd, out = take(3)
    a, at, dyt, hid, dgate, dup = take(6)
    if not final:
        dag, dau = take(2)
    else:
        mine, theirs, sq_send, sq_recv = take(4)
    p = Place(n)
    if final:
        greet([lax.rem(p.me + k, n) for k in range(1, n)])
    else:
        greet([p.device(1), p.device(-1), p.partner])
    sc = Scatter(p, take(8), take(6))
    tokens, d = h.shape
    block = hid.shape[1]
    blocks = p.chips

    def prepare(i, _):
        rows = pl.ds(pl.multiple_of(i * 256, 256), 256)
        one = normed(h[rows, :].astype(F32))
        a[rows, :] = one
        at[:, rows] = one.T
        dyt[:, rows] = dy[rows, :].T
        if not final:
            dag[rows, :] = jnp.zeros((256, d), F32)
            dau[rows, :] = jnp.zeros((256, d), F32)
        return 0

    lax.fori_loop(0, tokens // 256, prepare, 0)

    def step(b, _):
        owner = sc.owner(b)

        @pl.when(b < blocks)
        def _():
            cols = pl.ds(pl.multiple_of(owner * block, block), block)

            def part(i, _):
                rows = pl.ds(pl.multiple_of(i * tile, tile), tile)
                one = a[rows, :]
                gate = dot(one, wg[:, cols])
                up = dot(one, wu[:, cols])
                by_hid = dot_nt(dy[rows, :], wd[cols, :]).astype(BF).astype(F32)
                s = jax.nn.sigmoid(gate)
                t = gate * s
                hid[rows, :] = (t * up).astype(BF)
                by_up = (t * by_hid).astype(BF)
                by_t = by_hid * up
                by_gate = (by_t * s + gate * by_t * (s * (1.0 - s))).astype(BF)
                dup[rows, :] = by_up
                dgate[rows, :] = by_gate
                if not final:
                    dag[rows, :] += dot_nt(by_gate, wg[:, cols])
                    dau[rows, :] += dot_nt(by_up, wu[:, cols])
                return 0

            lax.fori_loop(0, tokens // tile, part, 0)

        for s in range(4):
            @pl.when((b - 1 - s >= 0) & (b - 1 - s < blocks))
            def _(s=s):
                sc.stage(b - 1 - s, s)

        @pl.when((b - 5 >= 0) & (b - 5 < blocks))
        def _():
            sc.last(b - 5, out_gu, out_wd)

        @pl.when(b < blocks)
        def _():
            for_gate = dot(at[...], dgate[...])
            for_up = dot(at[...], dup[...])
            each = d // n
            for k in range(n):
                rows = slice(k * each, (k + 1) * each)
                sc.g_gu[b, k // 2, k % 2] = jnp.concatenate([for_gate[rows], for_up[rows]], 0).astype(BF)
            for_down = dot(dyt[...], hid[...]).T.astype(BF)
            sc.g_wd[b, 0] = for_down[: block // 2]
            sc.g_wd[b, 1] = for_down[block // 2 :]
            for c in sc.pair(b):
                c.start()

        return 0

    lax.fori_loop(0, blocks + 5, step, 0)

    if final:
        total = jnp.zeros((1, 1), F32)
        for ref in (out_gu, out_wd, *before):
            one = ref[...].astype(F32)
            total = total + jnp.sum(jnp.sum(one * one, axis=1, keepdims=True), axis=0, keepdims=True)
        mine[...] = jnp.broadcast_to(total, mine.shape)

        def to(k):
            return remote(mine, theirs.at[k - 1], sq_send.at[k - 1], sq_recv.at[k - 1], lax.rem(p.me + k, n))

        for k in range(1, n):
            to(k).start()
        for k in range(1, n):
            to(k).wait_recv()
        acc = mine[...]
        for k in range(1, n):
            acc = acc + theirs[k - 1]
        out[...] = acc
        for k in range(1, n):
            to(k).wait_send()
    else:
        def close(i, _):
            rows = pl.ds(pl.multiple_of(i * 256, 256), 256)
            wide = h[rows, :].astype(F32)
            mean = jnp.mean(wide * wide, -1, keepdims=True) + 1e-6
            scale = lax.rsqrt(mean)
            by_a = (dag[rows, :].astype(BF) + dau[rows, :].astype(BF)).astype(F32)
            inner = jnp.sum(wide * by_a, -1, keepdims=True)
            by_h = by_a * scale + (inner * (-0.5 * scale / mean) / d) * (2.0 * wide)
            out[rows, :] = dy[rows, :] + by_h.astype(BF)
            return 0

        lax.fori_loop(0, tokens // 256, close, 0)
    sc.drain()


def adamw(w, m, v, g):
    m = 0.9 * m + 0.1 * g
    v = 0.95 * v + 0.05 * g * g
    step = m * lax.rsqrt(v + 1e-8) + 0.1 * w
    return (w - 0.02 * step).astype(BF), m, v


def solution(mesh):
    n = mesh.shape["dp"]
    any_, vmem = pl.BlockSpec(memory_space=pl.ANY), pl.BlockSpec(memory_space=pltpu.VMEM)

    def params(k):
        return pltpu.CompilerParams(collective_id=k, has_side_effects=True, vmem_limit_bytes=VMEM_LIMIT)

    def shape(*s, dtype=BF):
        return jax.ShapeDtypeStruct(s, dtype)

    def step(x, dy, *arrays):
        weights, m, v = (arrays[i : i + 3] for i in (0, 3, 6))
        wg, wu, wd = weights
        x, dy = x[0], dy[0]
        tokens, d = x.shape
        rows, ff = wg.shape[1:]
        deep = wd.shape[1]
        fulls = [shape(n, rows, ff), shape(n, rows, ff), shape(n, deep, d)]
        flat = lambda f: (f[0].reshape(d, ff), f[1].reshape(d, ff), f[2].reshape(ff, d))
        first = pl.pallas_call(
            functools.partial(gather_kernel, n, 0),
            out_shape=fulls,
            in_specs=[any_] * 3,
            out_specs=[vmem] * 3,
            scratch_shapes=Gather.sems(n, 3),
            compiler_params=params(0),
            name="gather0",
        )(wg, wu, wd)
        w0 = flat(first)
        h, *second = pl.pallas_call(
            functools.partial(forward_kernel, n, 1, 256),
            out_shape=[shape(tokens, d)] + fulls,
            in_specs=[vmem] * 4 + [any_] * 3,
            out_specs=[vmem] * 4,
            scratch_shapes=Gather.sems(n, 3),
            compiler_params=params(1),
            name="forward0",
        )(x, *w0, wg, wu, wd)
        w1 = flat(second)

        block = ff // (n // 2)
        gu, wdb = (2 * rows, block), (deep, d)
        common = [
            pltpu.VMEM((tokens, d), BF),
            pltpu.VMEM((d, tokens), BF),
            pltpu.VMEM((d, tokens), BF),
            pltpu.VMEM((tokens, block), BF),
            pltpu.VMEM((tokens, block), BF),
            pltpu.VMEM((tokens, block), BF),
        ]
        gu1, wd1, dh = pl.pallas_call(
            functools.partial(backward_kernel, n, 512, False),
            out_shape=[shape(2 * rows, ff), shape(deep, d), shape(tokens, d)],
            in_specs=[vmem] * 5,
            out_specs=[vmem] * 3,
            scratch_shapes=common + [pltpu.VMEM((tokens, d), F32)] * 2 + Scatter.scratch(n, gu, wdb),
            compiler_params=params(2),
            name="backward1",
        )(h, dy, *w1)
        gu0, wd0, squares = pl.pallas_call(
            functools.partial(backward_kernel, n, 512, True),
            out_shape=[shape(2 * rows, ff), shape(deep, d), shape(8, 128, dtype=F32)],
            in_specs=[vmem] * 7,
            out_specs=[vmem] * 3,
            scratch_shapes=common
            + [
                pltpu.VMEM((8, 128), F32),
                pltpu.VMEM((n - 1, 8, 128), F32),
                pltpu.SemaphoreType.DMA((n - 1,)),
                pltpu.SemaphoreType.DMA((n - 1,)),
            ]
            + Scatter.scratch(n, gu, wdb),
            compiler_params=params(3),
            name="backward0",
        )(x, dh, *w0, gu1, wd1)

        gradients = [
            jnp.stack([gu0[:rows], gu1[:rows]]),
            jnp.stack([gu0[rows:], gu1[rows:]]),
            jnp.stack([wd0, wd1]),
        ]
        count = n * sum(g.size for g in gradients)
        factor = jnp.minimum(1.0, 0.5 * lax.rsqrt(squares[0, 0] / count + 1e-30))
        new = [adamw(w.astype(F32), m, v, g.astype(F32) * factor) for w, m, v, g in zip(weights, m, v, gradients, strict=True)]
        return tuple(one[which] for which in range(3) for one in new)

    states, cut = P(("rep", "dp"), None, None), P(None, "dp", None)
    return jax.shard_map(
        step,
        mesh=mesh,
        in_specs=(states, states) + (cut,) * 9,
        out_specs=(P("rep", "dp", None),) * 9,
        check_vma=False,
    )
```

```python
import functools

import jax
import jax.numpy as jnp
from jax import lax
from jax.experimental import pallas as pl
from jax.experimental.pallas import tpu as pltpu
from jax.sharding import PartitionSpec as P

BF, F32 = jnp.bfloat16, jnp.float32
MESH = pl.DeviceIdType.MESH
VMEM_LIMIT = 67_000_000
NT = (((1,), (1,)), ((), ()))


def normed(wide):
    scale = lax.rsqrt(jnp.mean(wide * wide, -1, keepdims=True) + 1e-6)
    return (wide * scale).astype(BF)


def dot(a, b):
    return jnp.dot(a, b, preferred_element_type=F32)


def dot_nt(a, b):
    return lax.dot_general(a, b, NT, preferred_element_type=F32)


class Place:
    def __init__(self, n):
        self.n, self.chips = n, n // 2
        self.me = lax.axis_index("dp")
        self.core = lax.rem(self.me, 2)
        self.chip = lax.div(self.me, 2)
        self.partner = self.chip * 2 + (1 - self.core)

    def at(self, offset):
        return lax.rem(self.chip + offset + self.chips, self.chips)

    def device(self, offset):
        return self.at(offset) * 2 + self.core


def greet(devices):
    barrier = pltpu.get_barrier_semaphore()
    for device in devices:
        pl.semaphore_signal(barrier, inc=1, device_id={"dp": device}, device_id_type=MESH)
    pl.semaphore_wait(barrier, len(devices))


def remote(src, dst, send, recv, device):
    return pltpu.make_async_remote_copy(
        src_ref=src, dst_ref=dst, send_sem=send, recv_sem=recv, device_id={"dp": device}, device_id_type=MESH
    )


class Gather:
    def __init__(self, place, shards, fulls, sems):
        self.p, self.shards, self.fulls = place, shards, fulls
        self.local, self.rs, self.rr, self.ps, self.pr = sems
        self.half_hops = place.chips // 2

    @staticmethod
    def sems(n, pieces):
        return [
            pltpu.SemaphoreType.DMA((pieces,)),
            pltpu.SemaphoreType.DMA((pieces, 2, n // 4)),
            pltpu.SemaphoreType.DMA((pieces, 2, n // 4)),
            pltpu.SemaphoreType.DMA((pieces, n // 2)),
            pltpu.SemaphoreType.DMA((pieces, n // 2)),
        ]

    def half(self, ref, h):
        rows, cols = ref.shape
        if cols > rows * 8:
            return ref.at[:, h * (cols // 2) : (h + 1) * (cols // 2)]
        return ref.at[h * (rows // 2) : (h + 1) * (rows // 2), :]

    def hop(self, i, way, t):
        p, full = self.p, self.fulls[i]
        behind = (1 - t) if way == 0 else (t - 1)
        ref = full.at[p.device(behind)]
        if t == self.half_hops:
            ref = self.half(ref, way)
        return remote(ref, ref, self.rs.at[i, way, t - 1], self.rr.at[i, way, t - 1], p.device(1 if way == 0 else -1))

    def landed(self, i, way, t):
        p, full = self.p, self.fulls[i]
        ref = full.at[p.device(-t if way == 0 else t)]
        if t == self.half_hops:
            ref = self.half(ref, way)
        return remote(ref, ref, self.rs.at[i, way, t - 1], self.rr.at[i, way, t - 1], p.device(1))

    def hand(self, i, k):
        p, full = self.p, self.fulls[i]
        offset = 0 if k == 0 else (-(k + 1) // 2 if k % 2 else k // 2)
        ref = full.at[p.device(offset)]
        return remote(ref, ref, self.ps.at[i, k], self.pr.at[i, k], p.partner)

    def handed(self, i, k):
        p, full = self.p, self.fulls[i]
        offset = 0 if k == 0 else (-(k + 1) // 2 if k % 2 else k // 2)
        ref = full.at[p.at(offset) * 2 + (1 - p.core)]
        return remote(ref, ref, self.ps.at[i, k], self.pr.at[i, k], p.partner)

    def begin(self):
        own = [pltpu.make_async_copy(s, f.at[self.p.me], self.local.at[i]) for i, (s, f) in enumerate(zip(self.shards, self.fulls))]
        for c in own:
            c.start()
        for i, c in enumerate(own):
            c.wait()
            self.hop(i, 0, 1).start()
            self.hop(i, 1, 1).start()
            self.hand(i, 0).start()

    def events(self):
        return [(t, i) for t in range(1, self.half_hops + 1) for i in range(len(self.fulls))]

    def forward(self, t, i):
        last = self.half_hops
        for way in range(2):
            self.landed(i, way, t).wait_recv()
            if t < last:
                self.hop(i, way, t + 1).start()
                self.hand(i, 2 * t - 1 + way).start()
        if t == last:
            self.hand(i, 2 * last - 1).start()

    def finish(self):
        for i in range(len(self.fulls)):
            for k in range(self.p.chips):
                self.handed(i, k).wait_recv()
        for i in range(len(self.fulls)):
            for k in range(self.p.chips):
                self.hand(i, k).wait_send()
            for way in range(2):
                for t in range(1, self.half_hops + 1):
                    self.hop(i, way, t).wait_send()


def gather_kernel(n, layer, wg, wu, wd, fg, fu, fd, *sems):
    p = Place(n)
    greet([p.device(1), p.device(-1), p.partner])
    g = Gather(p, [w.at[layer] for w in (wg, wu, wd)], [fg, fu, fd], sems)
    g.begin()
    for t, i in g.events():
        g.forward(t, i)
    g.finish()


def forward_kernel(n, layer, tile, x, wg, wu, wd, sg, su, sd, y, fg, fu, fd, *sems):
    p = Place(n)
    greet([p.device(1), p.device(-1), p.partner])
    g = Gather(p, [w.at[layer] for w in (sg, su, sd)], [fg, fu, fd], sems)
    g.begin()
    events = g.events()
    tiles = x.shape[0] // tile
    ff = wg.shape[1]
    width = 512

    def body(i, _):
        rows = pl.ds(pl.multiple_of(i * tile, tile), tile)
        h = x[rows, :]
        a = normed(h.astype(F32))
        out = None
        for c in range(0, ff, width):
            gate = dot(a, wg[:, c : c + width])
            up = dot(a, wu[:, c : c + width])
            hid = (gate * jax.nn.sigmoid(gate) * up).astype(BF)
            term = dot(hid, wd[c : c + width, :])
            out = term if out is None else out + term
        y[rows, :] = h + out.astype(BF)
        for k, (t, j) in enumerate(events):
            @pl.when(i == k)
            def _(t=t, j=j):
                g.forward(t, j)
        return 0

    lax.fori_loop(0, tiles, body, 0)
    for t, j in events[tiles:]:
        g.forward(t, j)
    g.finish()


class Scatter:
    def __init__(self, place, refs, sems):
        self.p = place
        self.g_gu, self.q_gu, self.s_gu, self.r_gu, self.g_wd, self.q_wd, self.s_wd, self.r_wd = refs
        self.ss_gu, self.sr_gu, self.ss_wd, self.sr_wd, self.ps, self.pr = sems

    @staticmethod
    def scratch(n, gu, wd):
        chips = n // 2
        return [
            pltpu.VMEM((chips, chips, 2) + gu, BF),
            pltpu.VMEM((chips, chips) + gu, BF),
            pltpu.VMEM((chips, 2, 4) + gu, BF),
            pltpu.VMEM((chips, 2, 4) + gu, BF),
            pltpu.VMEM((chips, 2) + wd, BF),
            pltpu.VMEM((chips,) + wd, BF),
            pltpu.VMEM((chips, 2) + wd, BF),
            pltpu.VMEM((chips, 2) + wd, BF),
            pltpu.SemaphoreType.DMA((chips, 2, 4)),
            pltpu.SemaphoreType.DMA((chips, 2, 4)),
            pltpu.SemaphoreType.DMA((chips, 2)),
            pltpu.SemaphoreType.DMA((chips, 2)),
            pltpu.SemaphoreType.DMA((chips, 2)),
            pltpu.SemaphoreType.DMA((chips, 2)),
        ]

    def owner(self, b):
        half = self.p.chips // 2
        b = lax.rem(b, self.p.chips)
        return lax.div(b, 2) + half * lax.rem(b, 2)

    def pair(self, b):
        p = self.p
        return [
            remote(self.g_gu.at[b, :, 1 - p.core], self.q_gu.at[b], self.ps.at[b, 0], self.pr.at[b, 0], p.partner),
            remote(self.g_wd.at[b, 1 - p.core], self.q_wd.at[b], self.ps.at[b, 1], self.pr.at[b, 1], p.partner),
        ]

    def own_gu(self, b, chip, cols):
        return self.g_gu[b, chip, self.p.core, :, cols].astype(F32) + self.q_gu[b, chip, :, cols].astype(F32)

    def own_wd(self, b, rows):
        return self.g_wd[b, self.p.core, rows, :].astype(F32) + self.q_wd[b, rows, :].astype(F32)

    def gu_copy(self, b, way, s):
        src, dst = self.s_gu.at[b, way, s], self.r_gu.at[b, way, s]
        if s == 0:
            w = src.shape[1] // 2
            src, dst = (r.at[:, way * w : (way + 1) * w] for r in (src, dst))
        return remote(src, dst, self.ss_gu.at[b, way, s], self.sr_gu.at[b, way, s], self.p.device(1 if way == 0 else -1))

    def wd_copy(self, b, way, first):
        src, dst = self.s_wd.at[b, way], self.r_wd.at[b, way]
        if first:
            h = src.shape[0] // 2
            src, dst = (r.at[way * h : (way + 1) * h, :] for r in (src, dst))
        return remote(src, dst, self.ss_wd.at[b, way], self.sr_wd.at[b, way], self.p.device(1 if way == 0 else -1))

    def stage(self, chain, s):
        p = self.p
        b = lax.rem(chain, p.chips)
        if s == 0:
            for c in self.pair(b):
                c.wait_recv()
        width, height = self.g_gu.shape[-1] // 2, self.g_wd.shape[-2] // 2
        for way in range(2):
            far = 4 - s
            chip = p.at(far if way == 0 else -far)
            if s > 0:
                self.gu_copy(b, way, s - 1).wait_recv()
            for h in range(2):
                cols = slice(h * width, (h + 1) * width)
                if s == 0 and h != way:
                    continue
                term = self.own_gu(b, chip, cols)
                if s > 1 or (s == 1 and h == way):
                    term = term + self.r_gu[b, way, s - 1, :, cols].astype(F32)
                self.s_gu[b, way, s, :, cols] = term.astype(BF)
            self.gu_copy(b, way, s).start()

        owner = self.owner(b)
        for way in range(2):
            far = 4 - s

            @pl.when(owner == p.at(far if way == 0 else -far))
            def _(way=way):
                if s > 0:
                    self.wd_copy(b, way, s == 1).wait_recv()
                for h in range(2):
                    rows = slice(h * height, (h + 1) * height)
                    if s == 0 and h != way:
                        continue
                    term = self.own_wd(b, rows)
                    if s > 1 or (s == 1 and h == way):
                        term = term + self.r_wd[b, way, rows, :].astype(F32)
                    self.s_wd[b, way, rows, :] = term.astype(BF)
                self.wd_copy(b, way, s == 0).start()

    def last(self, chain, out_gate, out_up, out_wd):
        p = self.p
        b = lax.rem(chain, p.chips)
        layer = out_wd.shape[0] - 1 - lax.div(chain, p.chips)
        owner = self.owner(b)
        full = slice(None)
        width = self.g_gu.shape[-1]
        rows = self.g_gu.shape[-2] // 2
        for way in range(2):
            self.gu_copy(b, way, 3).wait_recv()
        total = self.own_gu(b, p.chip, full) + self.r_gu[b, 0, 3].astype(F32) + self.r_gu[b, 1, 3].astype(F32)
        cols = pl.ds(pl.multiple_of(owner * width, width), width)
        out_gate[layer, :, cols] = total[:rows].astype(BF)
        out_up[layer, :, cols] = total[rows:].astype(BF)

        @pl.when(owner == p.chip)
        def _():
            for way in range(2):
                self.wd_copy(b, way, False).wait_recv()
            out_wd[layer] = (self.own_wd(b, full) + self.r_wd[b, 0].astype(F32) + self.r_wd[b, 1].astype(F32)).astype(BF)

    def drain(self, chain):
        p = self.p
        b = lax.rem(chain, p.chips)
        for c in self.pair(b):
            c.wait_send()
        owner = self.owner(b)
        for way in range(2):
            for s in range(4):
                self.gu_copy(b, way, s).wait_send()
                far = 4 - s

                @pl.when(owner == p.at(far if way == 0 else -far))
                def _(way=way, s=s):
                    self.wd_copy(b, way, s == 0).wait_send()


def backward_kernel(n, tile, x, h, dy, wg0, wu0, wd0, wg1, wu1, wd1, out_gate, out_up, out_wd, out, *refs):
    refs = list(refs)
    take = lambda k: [refs.pop(0) for _ in range(k)]
    hs, by, a, at, dyt, hid, dgate, dup, dag, dau, bg, bu, bd, mine, theirs = take(15)
    in_sem, w_sem, sq_send, sq_recv = take(4)
    p = Place(n)
    sc = Scatter(p, take(8), take(6))
    tokens, d = by.shape
    block = hid.shape[1]
    blocks = p.chips
    chains = 2 * blocks
    step_rows = 256

    loads = [
        pltpu.make_async_copy(h, hs.at[1], in_sem.at[0]),
        pltpu.make_async_copy(dy, by, in_sem.at[1]),
        pltpu.make_async_copy(x, hs.at[0], in_sem.at[2]),
    ]

    def fetch(b, weights):
        cols = pl.ds(pl.multiple_of(sc.owner(b) * block, block), block)
        slot = lax.rem(b, 2)
        g, u, w = weights
        return [
            pltpu.make_async_copy(g.at[:, cols], bg.at[slot], w_sem.at[slot, 0]),
            pltpu.make_async_copy(u.at[:, cols], bu.at[slot], w_sem.at[slot, 1]),
            pltpu.make_async_copy(w.at[cols, :], bd.at[slot], w_sem.at[slot, 2]),
        ]

    first, second = (wg1, wu1, wd1), (wg0, wu0, wd0)
    for c in loads + fetch(0, first):
        c.start()
    greet([lax.rem(p.me + k, n) for k in range(1, n)])
    for c in loads[:2]:
        c.wait()

    def prepare(i, _):
        rows = pl.ds(pl.multiple_of(i * step_rows, step_rows), step_rows)
        one = normed(hs[1, rows, :].astype(F32))
        a[rows, :] = one
        at[:, rows] = one.T
        dyt[:, rows] = by[rows, :].T
        dag[rows, :] = jnp.zeros((step_rows, d), F32)
        dau[rows, :] = jnp.zeros((step_rows, d), F32)
        return 0

    lax.fori_loop(0, tokens // step_rows, prepare, 0)

    def turn(i, _):
        rows = pl.ds(pl.multiple_of(i * step_rows, step_rows), step_rows)
        wide = hs[1, rows, :].astype(F32)
        mean = jnp.mean(wide * wide, -1, keepdims=True) + 1e-6
        scale = lax.rsqrt(mean)
        by_a = (dag[rows, :].astype(BF) + dau[rows, :].astype(BF)).astype(F32)
        inner = jnp.sum(wide * by_a, -1, keepdims=True)
        by_h = by_a * scale + (inner * (-0.5 * scale / mean) / d) * (2.0 * wide)
        new = by[rows, :] + by_h.astype(BF)
        by[rows, :] = new
        dyt[:, rows] = new.T
        one = normed(hs[0, rows, :].astype(F32))
        a[rows, :] = one
        at[:, rows] = one.T
        return 0

    def part(slot, with_da, i, _):
        rows = pl.ds(pl.multiple_of(i * tile, tile), tile)
        one = a[rows, :]
        gate = dot(one, bg[slot])
        up = dot(one, bu[slot])
        by_hid = dot_nt(by[rows, :], bd[slot]).astype(BF).astype(F32)
        s = jax.nn.sigmoid(gate)
        t = gate * s
        hid[rows, :] = (t * up).astype(BF)
        by_up = (t * by_hid).astype(BF)
        by_t = by_hid * up
        by_gate = (by_t * s + gate * by_t * (s * (1.0 - s))).astype(BF)
        dup[rows, :] = by_up
        dgate[rows, :] = by_gate
        if with_da:
            dag[rows, :] += dot_nt(by_gate, bg[slot])
            dau[rows, :] += dot_nt(by_up, bu[slot])
        return 0

    def step(b, _):
        slot = lax.rem(b, 2)

        @pl.when(b < blocks - 1)
        def _():
            for c in fetch(b + 1, first):
                c.start()

        @pl.when((b >= blocks - 1) & (b < chains - 1))
        def _():
            for c in fetch(b + 1, second):
                c.start()

        @pl.when(b == blocks)
        def _():
            loads[2].wait()
            lax.fori_loop(0, tokens // step_rows, turn, 0)

        @pl.when(b < blocks)
        def _():
            for c in fetch(b, first):
                c.wait()
            lax.fori_loop(0, tokens // tile, functools.partial(part, slot, True), 0)

        @pl.when((b >= blocks) & (b < chains))
        def _():
            for c in fetch(b, second):
                c.wait()
            lax.fori_loop(0, tokens // tile, functools.partial(part, slot, False), 0)

        for s in range(4):
            @pl.when((b - 1 - s >= 0) & (b - 1 - s < chains))
            def _(s=s):
                sc.stage(b - 1 - s, s)

        @pl.when((b - 5 >= 0) & (b - 5 < chains))
        def _():
            sc.last(b - 5, out_gate, out_up, out_wd)

        @pl.when((b - 6 >= 0) & (b - 6 < chains))
        def _():
            sc.drain(b - 6)

        @pl.when(b < chains)
        def _():
            q = lax.rem(b, blocks)
            for_gate = dot(at[...], dgate[...])
            for_up = dot(at[...], dup[...])
            each = d // n
            for k in range(n):
                rows = slice(k * each, (k + 1) * each)
                sc.g_gu[q, k // 2, k % 2] = jnp.concatenate([for_gate[rows], for_up[rows]], 0).astype(BF)
            for_down = dot(dyt[...], hid[...]).T.astype(BF)
            sc.g_wd[q, 0] = for_down[: block // 2]
            sc.g_wd[q, 1] = for_down[block // 2 :]
            for c in sc.pair(q):
                c.start()

        return 0

    lax.fori_loop(0, chains + 6, step, 0)

    total = jnp.zeros((1, 1), F32)
    for ref in (out_gate, out_up, out_wd):
        for k in range(2):
            one = ref[k].astype(F32)
            total = total + jnp.sum(jnp.sum(one * one, axis=1, keepdims=True), axis=0, keepdims=True)
    mine[...] = jnp.broadcast_to(total, mine.shape)

    def to(k):
        return remote(mine, theirs.at[k - 1], sq_send.at[k - 1], sq_recv.at[k - 1], lax.rem(p.me + k, n))

    for k in range(1, n):
        to(k).start()
    for k in range(1, n):
        to(k).wait_recv()
    acc = mine[...]
    for k in range(1, n):
        acc = acc + theirs[k - 1]
    out[...] = acc
    for k in range(1, n):
        to(k).wait_send()


def adamw(w, m, v, g):
    m = 0.9 * m + 0.1 * g
    v = 0.95 * v + 0.05 * g * g
    step = m * lax.rsqrt(v + 1e-8) + 0.1 * w
    return (w - 0.02 * step).astype(BF), m, v


def solution(mesh):
    n = mesh.shape["dp"]
    any_, vmem = pl.BlockSpec(memory_space=pl.ANY), pl.BlockSpec(memory_space=pltpu.VMEM)

    def params(k):
        return pltpu.CompilerParams(collective_id=k, has_side_effects=True, vmem_limit_bytes=VMEM_LIMIT)

    def shape(*s, dtype=BF):
        return jax.ShapeDtypeStruct(s, dtype)

    def step(x, dy, *arrays):
        weights, m, v = (arrays[i : i + 3] for i in (0, 3, 6))
        wg, wu, wd = weights
        x, dy = x[0], dy[0]
        tokens, d = x.shape
        rows, ff = wg.shape[1:]
        deep = wd.shape[1]
        fulls = [shape(n, rows, ff), shape(n, rows, ff), shape(n, deep, d)]
        flat = lambda f: (f[0].reshape(d, ff), f[1].reshape(d, ff), f[2].reshape(ff, d))
        first = pl.pallas_call(
            functools.partial(gather_kernel, n, 0),
            out_shape=fulls,
            in_specs=[any_] * 3,
            out_specs=[vmem] * 3,
            scratch_shapes=Gather.sems(n, 3),
            compiler_params=params(0),
            name="gather0",
        )(wg, wu, wd)
        w0 = flat(first)
        h, *second = pl.pallas_call(
            functools.partial(forward_kernel, n, 1, 256),
            out_shape=[shape(tokens, d)] + fulls,
            in_specs=[vmem] * 4 + [any_] * 3,
            out_specs=[vmem] * 4,
            scratch_shapes=Gather.sems(n, 3),
            compiler_params=params(1),
            name="forward0",
        )(x, *w0, wg, wu, wd)
        w1 = flat(second)

        block = ff // (n // 2)
        *gradients, squares = pl.pallas_call(
            functools.partial(backward_kernel, n, 512),
            out_shape=[shape(2, rows, ff), shape(2, rows, ff), shape(2, deep, d), shape(8, 128, dtype=F32)],
            in_specs=[any_] * 9,
            out_specs=[vmem] * 4,
            scratch_shapes=[
                pltpu.VMEM((2, tokens, d), BF),
                pltpu.VMEM((tokens, d), BF),
                pltpu.VMEM((tokens, d), BF),
                pltpu.VMEM((d, tokens), BF),
                pltpu.VMEM((d, tokens), BF),
                pltpu.VMEM((tokens, block), BF),
                pltpu.VMEM((tokens, block), BF),
                pltpu.VMEM((tokens, block), BF),
                pltpu.VMEM((tokens, d), F32),
                pltpu.VMEM((tokens, d), F32),
                pltpu.VMEM((2, d, block), BF),
                pltpu.VMEM((2, d, block), BF),
                pltpu.VMEM((2, block, d), BF),
                pltpu.VMEM((8, 128), F32),
                pltpu.VMEM((n - 1, 8, 128), F32),
                pltpu.SemaphoreType.DMA((3,)),
                pltpu.SemaphoreType.DMA((2, 3)),
                pltpu.SemaphoreType.DMA((n - 1,)),
                pltpu.SemaphoreType.DMA((n - 1,)),
            ]
            + Scatter.scratch(n, (2 * rows, block), (deep, d)),
            compiler_params=params(2),
            name="backward",
        )(x, h, dy, *w0, *w1)

        count = n * sum(g.size for g in gradients)
        factor = jnp.minimum(1.0, 0.5 * lax.rsqrt(squares[0, 0] / count + 1e-30))
        new = [adamw(w.astype(F32), m, v, g.astype(F32) * factor) for w, m, v, g in zip(weights, m, v, gradients, strict=True)]
        return tuple(one[which] for which in range(3) for one in new)

    states, cut = P(("rep", "dp"), None, None), P(None, "dp", None)
    return jax.shard_map(
        step,
        mesh=mesh,
        in_specs=(states, states) + (cut,) * 9,
        out_specs=(P("rep", "dp", None),) * 9,
        check_vma=False,
    )
```

```python
import functools

import jax
import jax.numpy as jnp
from jax import lax
from jax.experimental import pallas as pl
from jax.experimental.pallas import tpu as pltpu
from jax.sharding import PartitionSpec as P

BF, F32 = jnp.bfloat16, jnp.float32
MESH = pl.DeviceIdType.MESH
VMEM_LIMIT = 67_000_000
NT = (((1,), (1,)), ((), ()))


def normed(wide):
    scale = lax.rsqrt(jnp.mean(wide * wide, -1, keepdims=True) + 1e-6)
    return (wide * scale).astype(BF)


def dot(a, b):
    return jnp.dot(a, b, preferred_element_type=F32)


def dot_nt(a, b):
    return lax.dot_general(a, b, NT, preferred_element_type=F32)


class Place:
    def __init__(self, n):
        self.n, self.chips = n, n // 2
        self.me = lax.axis_index("dp")
        self.core = lax.rem(self.me, 2)
        self.chip = lax.div(self.me, 2)
        self.partner = self.chip * 2 + (1 - self.core)

    def at(self, offset):
        return lax.rem(self.chip + offset + self.chips, self.chips)

    def device(self, offset):
        return self.at(offset) * 2 + self.core


def greet(devices):
    barrier = pltpu.get_barrier_semaphore()
    for device in devices:
        pl.semaphore_signal(barrier, inc=1, device_id={"dp": device}, device_id_type=MESH)
    pl.semaphore_wait(barrier, len(devices))


def remote(src, dst, send, recv, device):
    return pltpu.make_async_remote_copy(
        src_ref=src, dst_ref=dst, send_sem=send, recv_sem=recv, device_id={"dp": device}, device_id_type=MESH
    )


class Gather:
    def __init__(self, place, shards, fulls, sems):
        self.p, self.shards, self.fulls = place, shards, fulls
        self.local, self.rs, self.rr, self.ps, self.pr = sems
        self.half_hops = place.chips // 2

    @staticmethod
    def sems(n, pieces):
        return [
            pltpu.SemaphoreType.DMA((pieces,)),
            pltpu.SemaphoreType.DMA((pieces, 2, n // 4)),
            pltpu.SemaphoreType.DMA((pieces, 2, n // 4)),
            pltpu.SemaphoreType.DMA((pieces, n // 2)),
            pltpu.SemaphoreType.DMA((pieces, n // 2)),
        ]

    def half(self, ref, h):
        rows, cols = ref.shape
        if cols > rows * 8:
            return ref.at[:, h * (cols // 2) : (h + 1) * (cols // 2)]
        return ref.at[h * (rows // 2) : (h + 1) * (rows // 2), :]

    def slot(self, i, device):
        rows = self.fulls[i].shape[0] // self.p.n
        return self.fulls[i].at[pl.ds(pl.multiple_of(device * rows, rows), rows), :]

    def hop(self, i, way, t):
        p = self.p
        behind = (1 - t) if way == 0 else (t - 1)
        ref = self.slot(i, p.device(behind))
        if t == self.half_hops:
            ref = self.half(ref, way)
        return remote(ref, ref, self.rs.at[i, way, t - 1], self.rr.at[i, way, t - 1], p.device(1 if way == 0 else -1))

    def landed(self, i, way, t):
        p = self.p
        ref = self.slot(i, p.device(-t if way == 0 else t))
        if t == self.half_hops:
            ref = self.half(ref, way)
        return remote(ref, ref, self.rs.at[i, way, t - 1], self.rr.at[i, way, t - 1], p.device(1))

    def hand(self, i, k):
        p = self.p
        offset = 0 if k == 0 else (-(k + 1) // 2 if k % 2 else k // 2)
        ref = self.slot(i, p.device(offset))
        return remote(ref, ref, self.ps.at[i, k], self.pr.at[i, k], p.partner)

    def handed(self, i, k):
        p = self.p
        offset = 0 if k == 0 else (-(k + 1) // 2 if k % 2 else k // 2)
        ref = self.slot(i, p.at(offset) * 2 + (1 - p.core))
        return remote(ref, ref, self.ps.at[i, k], self.pr.at[i, k], p.partner)

    def load(self):
        own = [pltpu.make_async_copy(s, self.slot(i, self.p.me), self.local.at[i]) for i, s in enumerate(self.shards)]
        for c in own:
            c.start()
        return own

    def begin(self, own):
        for i, c in enumerate(own):
            c.wait()
            self.hop(i, 0, 1).start()
            self.hop(i, 1, 1).start()
            self.hand(i, 0).start()

    def events(self):
        return [(t, i) for t in range(1, self.half_hops + 1) for i in range(len(self.fulls))]

    def forward(self, t, i):
        last = self.half_hops
        for way in range(2):
            self.landed(i, way, t).wait_recv()
            if t < last:
                self.hop(i, way, t + 1).start()
                self.hand(i, 2 * t - 1 + way).start()
        if t == last:
            self.hand(i, 2 * last - 1).start()

    def arrive(self):
        for i in range(len(self.fulls)):
            for k in range(self.p.chips):
                self.handed(i, k).wait_recv()

    def drain(self):
        for i in range(len(self.fulls)):
            for k in range(self.p.chips):
                self.hand(i, k).wait_send()
            for way in range(2):
                for t in range(1, self.half_hops + 1):
                    self.hop(i, way, t).wait_send()


def forward_kernel(n, tile, x, sg, su, sd, y, fg, fu, fd, gg, gu, gd, *sems):
    p = Place(n)
    per = len(sems) // 2
    first = Gather(p, [w.at[0] for w in (sg, su, sd)], [fg, fu, fd], sems[:per])
    second = Gather(p, [w.at[1] for w in (sg, su, sd)], [gg, gu, gd], sems[per:])
    own = first.load(), second.load()
    greet([p.device(1), p.device(-1), p.partner])
    first.begin(own[0])
    events = first.events()
    for t, i in events:
        if (t, i) == (first.half_hops, 0):
            second.begin(own[1])
        first.forward(t, i)
    first.arrive()
    tiles = x.shape[0] // tile
    ff = fg.shape[1]
    width = 512

    def body(i, _):
        rows = pl.ds(pl.multiple_of(i * tile, tile), tile)
        h = x[rows, :]
        a = normed(h.astype(F32))
        out = None
        for c in range(0, ff, width):
            gate = dot(a, fg[:, c : c + width])
            up = dot(a, fu[:, c : c + width])
            hid = (gate * jax.nn.sigmoid(gate) * up).astype(BF)
            term = dot(hid, fd[c : c + width, :])
            out = term if out is None else out + term
        y[rows, :] = h + out.astype(BF)
        for k, (t, j) in enumerate(events):
            @pl.when(i == k)
            def _(t=t, j=j):
                second.forward(t, j)
        return 0

    lax.fori_loop(0, tiles, body, 0)
    for t, j in events[tiles:]:
        second.forward(t, j)
    second.arrive()
    first.drain()
    second.drain()


class Scatter:
    def __init__(self, place, refs, sems):
        self.p = place
        self.g_gu, self.q_gu, self.s_gu, self.r_gu, self.g_wd, self.q_wd, self.s_wd, self.r_wd = refs
        self.ss_gu, self.sr_gu, self.ss_wd, self.sr_wd, self.ps, self.pr = sems

    @staticmethod
    def scratch(n, gu, wd):
        chips = n // 2
        return [
            pltpu.VMEM((chips, chips, 2) + gu, BF),
            pltpu.VMEM((chips, chips) + gu, BF),
            pltpu.VMEM((chips, 2, 4) + gu, BF),
            pltpu.VMEM((chips, 2, 4) + gu, BF),
            pltpu.VMEM((chips, 2) + wd, BF),
            pltpu.VMEM((chips,) + wd, BF),
            pltpu.VMEM((chips, 2) + wd, BF),
            pltpu.VMEM((chips, 2) + wd, BF),
            pltpu.SemaphoreType.DMA((chips, 2, 4)),
            pltpu.SemaphoreType.DMA((chips, 2, 4)),
            pltpu.SemaphoreType.DMA((chips, 2)),
            pltpu.SemaphoreType.DMA((chips, 2)),
            pltpu.SemaphoreType.DMA((chips, 2)),
            pltpu.SemaphoreType.DMA((chips, 2)),
        ]

    def owner(self, b, core):
        return lax.rem(3 * b + core, self.p.chips)

    def columns(self, b):
        run = self.g_wd.shape[-2]
        return [pl.ds(pl.multiple_of((2 * self.owner(b, c) + c) * run, run), run) for c in range(2)]

    def pair(self, b):
        p = self.p
        return [
            remote(self.g_gu.at[b, :, 1 - p.core], self.q_gu.at[b], self.ps.at[b, 0], self.pr.at[b, 0], p.partner),
            remote(self.g_wd.at[b, 1 - p.core], self.q_wd.at[b], self.ps.at[b, 1], self.pr.at[b, 1], p.partner),
        ]

    def own_gu(self, b, chip, cols):
        return self.g_gu[b, chip, self.p.core, :, cols].astype(F32) + self.q_gu[b, chip, :, cols].astype(F32)

    def own_wd(self, b, rows):
        return self.g_wd[b, self.p.core, rows, :].astype(F32) + self.q_wd[b, rows, :].astype(F32)

    def gu_copy(self, b, way, s):
        src, dst = self.s_gu.at[b, way, s], self.r_gu.at[b, way, s]
        if s == 0:
            w = src.shape[1] // 2
            src, dst = (r.at[:, way * w : (way + 1) * w] for r in (src, dst))
        return remote(src, dst, self.ss_gu.at[b, way, s], self.sr_gu.at[b, way, s], self.p.device(1 if way == 0 else -1))

    def wd_copy(self, b, way, first):
        src, dst = self.s_wd.at[b, way], self.r_wd.at[b, way]
        if first:
            h = src.shape[0] // 2
            src, dst = (r.at[way * h : (way + 1) * h, :] for r in (src, dst))
        return remote(src, dst, self.ss_wd.at[b, way], self.sr_wd.at[b, way], self.p.device(1 if way == 0 else -1))

    def stage(self, chain, s):
        p = self.p
        b = lax.rem(chain, p.chips)
        if s == 0:
            for c in self.pair(b):
                c.wait_recv()
        width, height = self.g_gu.shape[-1] // 2, self.g_wd.shape[-2] // 2
        for way in range(2):
            far = 4 - s
            chip = p.at(far if way == 0 else -far)
            if s > 0:
                self.gu_copy(b, way, s - 1).wait_recv()
            for h in range(2):
                cols = slice(h * width, (h + 1) * width)
                if s == 0 and h != way:
                    continue
                term = self.own_gu(b, chip, cols)
                if s > 1 or (s == 1 and h == way):
                    term = term + self.r_gu[b, way, s - 1, :, cols].astype(F32)
                self.s_gu[b, way, s, :, cols] = term.astype(BF)
            self.gu_copy(b, way, s).start()

        owner = self.owner(b, p.core)
        for way in range(2):
            far = 4 - s

            @pl.when(owner == p.at(far if way == 0 else -far))
            def _(way=way):
                if s > 0:
                    self.wd_copy(b, way, s == 1).wait_recv()
                for h in range(2):
                    rows = slice(h * height, (h + 1) * height)
                    if s == 0 and h != way:
                        continue
                    term = self.own_wd(b, rows)
                    if s > 1 or (s == 1 and h == way):
                        term = term + self.r_wd[b, way, rows, :].astype(F32)
                    self.s_wd[b, way, rows, :] = term.astype(BF)
                self.wd_copy(b, way, s == 0).start()

    def last(self, chain, out_gate, out_up, out_wd):
        p = self.p
        b = lax.rem(chain, p.chips)
        layer = out_wd.shape[0] - 1 - lax.div(chain, p.chips)
        owner = self.owner(b, p.core)
        full = slice(None)
        width = self.g_gu.shape[-1]
        rows = self.g_gu.shape[-2] // 2
        for way in range(2):
            self.gu_copy(b, way, 3).wait_recv()
        total = self.own_gu(b, p.chip, full) + self.r_gu[b, 0, 3].astype(F32) + self.r_gu[b, 1, 3].astype(F32)
        for c, cols in enumerate(self.columns(b)):
            run = slice(c * width // 2, (c + 1) * width // 2)
            out_gate[layer, :, cols] = total[:rows, run].astype(BF)
            out_up[layer, :, cols] = total[rows:, run].astype(BF)

        @pl.when(owner == p.chip)
        def _():
            for way in range(2):
                self.wd_copy(b, way, False).wait_recv()
            out_wd[layer] = (self.own_wd(b, full) + self.r_wd[b, 0].astype(F32) + self.r_wd[b, 1].astype(F32)).astype(BF)

    def drain(self, chain):
        p = self.p
        b = lax.rem(chain, p.chips)
        for c in self.pair(b):
            c.wait_send()
        owner = self.owner(b, p.core)
        for way in range(2):
            for s in range(4):
                self.gu_copy(b, way, s).wait_send()
                far = 4 - s

                @pl.when(owner == p.at(far if way == 0 else -far))
                def _(way=way, s=s):
                    self.wd_copy(b, way, s == 0).wait_send()


def backward_kernel(n, tile, x, h, dy, wg0, wu0, wd0, wg1, wu1, wd1, out_gate, out_up, out_wd, out, *refs):
    refs = list(refs)
    take = lambda k: [refs.pop(0) for _ in range(k)]
    hs, by, a, at, dyt, hid, dgate, dup, dag, dau, bg, bu, bd, mine, theirs = take(15)
    in_sem, w_sem, sq_send, sq_recv = take(4)
    p = Place(n)
    sc = Scatter(p, take(8), take(6))
    tokens, d = by.shape
    block = hid.shape[1]
    blocks = p.chips
    chains = 2 * blocks
    step_rows = 256

    loads = [
        pltpu.make_async_copy(h, hs.at[1], in_sem.at[0]),
        pltpu.make_async_copy(dy, by, in_sem.at[1]),
        pltpu.make_async_copy(x, hs.at[0], in_sem.at[2]),
    ]

    def fetch(b, weights):
        slot = lax.rem(b, 2)
        g, u, w = weights
        copies = []
        for c, cols in enumerate(sc.columns(b)):
            run = slice(c * block // 2, (c + 1) * block // 2)
            copies += [
                pltpu.make_async_copy(g.at[:, cols], bg.at[slot, :, run], w_sem.at[slot, c, 0]),
                pltpu.make_async_copy(u.at[:, cols], bu.at[slot, :, run], w_sem.at[slot, c, 1]),
                pltpu.make_async_copy(w.at[cols, :], bd.at[slot, run, :], w_sem.at[slot, c, 2]),
            ]
        return copies

    first, second = (wg1, wu1, wd1), (wg0, wu0, wd0)
    for c in loads + fetch(0, first):
        c.start()
    greet([lax.rem(p.me + k, n) for k in range(1, n)])
    for c in loads[:2]:
        c.wait()

    def prepare(i, _):
        rows = pl.ds(pl.multiple_of(i * step_rows, step_rows), step_rows)
        one = normed(hs[1, rows, :].astype(F32))
        a[rows, :] = one
        at[:, rows] = one.T
        dyt[:, rows] = by[rows, :].T
        dag[rows, :] = jnp.zeros((step_rows, d), F32)
        dau[rows, :] = jnp.zeros((step_rows, d), F32)
        return 0

    lax.fori_loop(0, tokens // step_rows, prepare, 0)

    def turn(i, _):
        rows = pl.ds(pl.multiple_of(i * step_rows, step_rows), step_rows)
        wide = hs[1, rows, :].astype(F32)
        mean = jnp.mean(wide * wide, -1, keepdims=True) + 1e-6
        scale = lax.rsqrt(mean)
        by_a = (dag[rows, :].astype(BF) + dau[rows, :].astype(BF)).astype(F32)
        inner = jnp.sum(wide * by_a, -1, keepdims=True)
        by_h = by_a * scale + (inner * (-0.5 * scale / mean) / d) * (2.0 * wide)
        new = by[rows, :] + by_h.astype(BF)
        by[rows, :] = new
        dyt[:, rows] = new.T
        one = normed(hs[0, rows, :].astype(F32))
        a[rows, :] = one
        at[:, rows] = one.T
        return 0

    def part(slot, with_da, i, _):
        rows = pl.ds(pl.multiple_of(i * tile, tile), tile)
        one = a[rows, :]
        gate = dot(one, bg[slot])
        up = dot(one, bu[slot])
        by_hid = dot_nt(by[rows, :], bd[slot]).astype(BF).astype(F32)
        s = jax.nn.sigmoid(gate)
        t = gate * s
        hid[rows, :] = (t * up).astype(BF)
        by_up = (t * by_hid).astype(BF)
        by_t = by_hid * up
        by_gate = (by_t * s + gate * by_t * (s * (1.0 - s))).astype(BF)
        dup[rows, :] = by_up
        dgate[rows, :] = by_gate
        if with_da:
            dag[rows, :] += dot_nt(by_gate, bg[slot])
            dau[rows, :] += dot_nt(by_up, bu[slot])
        return 0

    def step(b, _):
        slot = lax.rem(b, 2)

        @pl.when(b < blocks - 1)
        def _():
            for c in fetch(b + 1, first):
                c.start()

        @pl.when((b >= blocks - 1) & (b < chains - 1))
        def _():
            for c in fetch(b + 1, second):
                c.start()

        @pl.when(b == blocks)
        def _():
            loads[2].wait()
            lax.fori_loop(0, tokens // step_rows, turn, 0)

        @pl.when(b < blocks)
        def _():
            for c in fetch(b, first):
                c.wait()
            lax.fori_loop(0, tokens // tile, functools.partial(part, slot, True), 0)

        @pl.when((b >= blocks) & (b < chains))
        def _():
            for c in fetch(b, second):
                c.wait()
            lax.fori_loop(0, tokens // tile, functools.partial(part, slot, False), 0)

        for s in range(4):
            @pl.when((b - 1 - s >= 0) & (b - 1 - s < chains))
            def _(s=s):
                sc.stage(b - 1 - s, s)

        @pl.when((b - 5 >= 0) & (b - 5 < chains))
        def _():
            sc.last(b - 5, out_gate, out_up, out_wd)

        @pl.when((b - 6 >= 0) & (b - 6 < chains))
        def _():
            sc.drain(b - 6)

        @pl.when(b < chains)
        def _():
            q = lax.rem(b, blocks)
            for_gate = dot(at[...], dgate[...])
            for_up = dot(at[...], dup[...])
            each = d // n
            for k in range(n):
                rows = slice(k * each, (k + 1) * each)
                sc.g_gu[q, k // 2, k % 2] = jnp.concatenate([for_gate[rows], for_up[rows]], 0).astype(BF)
            for_down = dot(dyt[...], hid[...]).T.astype(BF)
            sc.g_wd[q, 0] = for_down[: block // 2]
            sc.g_wd[q, 1] = for_down[block // 2 :]
            for c in sc.pair(q):
                c.start()

        return 0

    lax.fori_loop(0, chains + 6, step, 0)

    total = jnp.zeros((1, 1), F32)
    for ref in (out_gate, out_up, out_wd):
        for k in range(2):
            one = ref[k].astype(F32)
            total = total + jnp.sum(jnp.sum(one * one, axis=1, keepdims=True), axis=0, keepdims=True)
    mine[...] = jnp.broadcast_to(total, mine.shape)

    def to(k):
        return remote(mine, theirs.at[k - 1], sq_send.at[k - 1], sq_recv.at[k - 1], lax.rem(p.me + k, n))

    for k in range(1, n):
        to(k).start()
    for k in range(1, n):
        to(k).wait_recv()
    acc = mine[...]
    for k in range(1, n):
        acc = acc + theirs[k - 1]
    out[...] = acc
    for k in range(1, n):
        to(k).wait_send()


def adamw(w, m, v, g):
    m = 0.9 * m + 0.1 * g
    v = 0.95 * v + 0.05 * g * g
    step = m * lax.rsqrt(v + 1e-8) + 0.1 * w
    return (w - 0.02 * step).astype(BF), m, v


def solution(mesh):
    n = mesh.shape["dp"]
    any_, vmem = pl.BlockSpec(memory_space=pl.ANY), pl.BlockSpec(memory_space=pltpu.VMEM)

    def params(k):
        return pltpu.CompilerParams(collective_id=k, has_side_effects=True, vmem_limit_bytes=VMEM_LIMIT)

    def shape(*s, dtype=BF):
        return jax.ShapeDtypeStruct(s, dtype)

    def step(x, dy, *arrays):
        weights, m, v = (arrays[i : i + 3] for i in (0, 3, 6))
        wg, wu, wd = weights
        x, dy = x[0], dy[0]
        tokens, d = x.shape
        rows, ff = wg.shape[1:]
        deep = wd.shape[1]
        fulls = [shape(d, ff), shape(d, ff), shape(ff, d)]
        h, *full = pl.pallas_call(
            functools.partial(forward_kernel, n, 256),
            out_shape=[shape(tokens, d)] + fulls + fulls,
            in_specs=[vmem] + [any_] * 3,
            out_specs=[vmem] * 7,
            scratch_shapes=Gather.sems(n, 3) * 2,
            compiler_params=params(1),
            name="forward",
        )(x, wg, wu, wd)
        w0, w1 = full[:3], full[3:]

        block = ff // (n // 2)
        *gradients, squares = pl.pallas_call(
            functools.partial(backward_kernel, n, 512),
            out_shape=[shape(2, rows, ff), shape(2, rows, ff), shape(2, deep, d), shape(8, 128, dtype=F32)],
            in_specs=[any_] * 9,
            out_specs=[vmem] * 4,
            scratch_shapes=[
                pltpu.VMEM((2, tokens, d), BF),
                pltpu.VMEM((tokens, d), BF),
                pltpu.VMEM((tokens, d), BF),
                pltpu.VMEM((d, tokens), BF),
                pltpu.VMEM((d, tokens), BF),
                pltpu.VMEM((tokens, block), BF),
                pltpu.VMEM((tokens, block), BF),
                pltpu.VMEM((tokens, block), BF),
                pltpu.VMEM((tokens, d), F32),
                pltpu.VMEM((tokens, d), F32),
                pltpu.VMEM((2, d, block), BF),
                pltpu.VMEM((2, d, block), BF),
                pltpu.VMEM((2, block, d), BF),
                pltpu.VMEM((8, 128), F32),
                pltpu.VMEM((n - 1, 8, 128), F32),
                pltpu.SemaphoreType.DMA((3,)),
                pltpu.SemaphoreType.DMA((2, 2, 3)),
                pltpu.SemaphoreType.DMA((n - 1,)),
                pltpu.SemaphoreType.DMA((n - 1,)),
            ]
            + Scatter.scratch(n, (2 * rows, block), (deep, d)),
            compiler_params=params(2),
            name="backward",
        )(x, h, dy, *w0, *w1)

        count = n * sum(g.size for g in gradients)
        factor = jnp.minimum(1.0, 0.5 * lax.rsqrt(squares[0, 0] / count + 1e-30))
        new = [adamw(w.astype(F32), m, v, g.astype(F32) * factor) for w, m, v, g in zip(weights, m, v, gradients, strict=True)]
        return tuple(one[which] for which in range(3) for one in new)

    states, cut = P(("rep", "dp"), None, None), P(None, "dp", None)
    return jax.shard_map(
        step,
        mesh=mesh,
        in_specs=(states, states) + (cut,) * 9,
        out_specs=(P("rep", "dp", None),) * 9,
        check_vma=False,
    )
```
